32 devices in a mesh: seq: 8 (over z, x), head: 4 (over y, core).
Axes of the slice: x: 2, y: 2, z: 4, core: 2. Of those that a mesh axis runs over, the one named last changes fastest.
Arguments:
- states: bfloat16 [4096, 2048], P('seq'), may hold values from -6 to 6
- inner_weight: bfloat16 [2048, 4096], P(None, 'head'), may hold values from -0.125 to 0.125
- gate_weight: bfloat16 [2048, 4096], P(None, 'head'), may hold values from -1 to 1
- state_weight: bfloat16 [2048, 256], replicated, may hold values from -0.125 to 0.125
- step_weight: bfloat16 [2048, 32], P(None, 'head'), may hold values from -0.125 to 0.125
- step_bias: float32 [32], P('head'), may hold values from -4 to -2
- decay_rate: float32 [32], P('head'), may hold values from 0 to 1
- skip_gain: float32 [32], P('head'), may hold values from 0.5 to 1.5
- conv_inner: float32 [4, 4096], P(None, 'head'), may hold values from -3 to 3
- conv_state: float32 [4, 256], replicated, may hold values from -3 to 3
- norm_gain: float32 [4096], P('head'), may hold values from 0.5 to 2
- value_weight: float32 [4096], P('head'), may hold values from -0.09375 to 0.09375
- rewards: float32 [4096], P('seq'), may hold values from -4 to 4
- done_flags: int32 [4096], P('seq'), may hold values from 0 to 1, as said below
- horizon: int32 [4096], P('seq'), may hold values from 1 to 8
Outputs:
- values: float32 [4096], P('seq')
- targets: float32 [4096], P('seq')
- value_loss: float32 [], replicated
The draws below stay inside these ranges and needn't reach their ends.
Inputs may be any that keep to these rules, and one draw needn't show every extreme that they name: `done_flags`: exactly one time step of the trajectory has an episode end.
All inputs are finite; a program needn't handle non-finite values.
Results may differ from the reference program's by a relative error of at most 0.007.
Values may be sent and summed in bfloat16 or wider, within the bound.
No kernel may reach another device: no remote copies, remote signals or barrier semaphores. Data moves between devices by JAX's collectives and lax.ppermute only.
A program may use at most 128 MiB of HBM per device.

```python
import math
import jax
import jax.numpy as jnp
from jax import lax

D = 2048
D_INNER = 4096
HEADS = 32
STATE = 128
KCONV = 4
NSTEP = 8
HDIM = 128
SEQ_LEN = 4096


def draw_gate_weight(key, part):
    column = jnp.arange(D_INNER, dtype=jnp.float32) / (D_INNER - 1)
    noise = jnp.clip(jax.random.normal(key, (D, D_INNER), jnp.float32), -4.0, 4.0)
    scales = 0.4 * 10.0 ** column
    return jnp.clip(noise * scales[None, :] / math.sqrt(D), -1.0, 1.0).astype(jnp.bfloat16)


def draw_decay_rate(key, part):
    order_key, slow_key, fast_key = jax.random.split(key, 3)
    ranking = jax.random.permutation(order_key, HEADS)
    slow_count = HEADS // 2
    slow_rate = jnp.exp(jax.random.uniform(slow_key, (HEADS,), jnp.float32, math.log(0.3), math.log(1.5))) / (0.1 * SEQ_LEN)
    fast_rate = jnp.exp(jax.random.uniform(fast_key, (HEADS,), jnp.float32, math.log(0.05), math.log(0.6)))
    return jnp.where(ranking < slow_count, slow_rate, fast_rate)


def draw_rewards(key, part):
    ramp = 1.0 + 2.0 * jnp.arange(SEQ_LEN, dtype=jnp.float32) / (SEQ_LEN - 1)
    noise = 0.2 * jnp.clip(jax.random.normal(key, (SEQ_LEN,), jnp.float32), -4.0, 4.0)
    return noise * ramp


def draw_done_flags(key, part):
    flag_key = jax.random.fold_in(key, 7)
    spread = max(1, 2 ** 30 // SEQ_LEN)
    scores = jax.random.randint(flag_key, (SEQ_LEN,), 0, spread, jnp.int32) * SEQ_LEN + jnp.arange(SEQ_LEN, dtype=jnp.int32)
    return (scores == jnp.max(scores)).astype(jnp.int32)


def touch_ends(result, key, low, largest):
    longest = result.shape.index(max(result.shape))
    spots = []
    for shift in (0, 1):
        where = [jax.random.randint(jax.random.fold_in(key, axis), (), 0, length) for axis, length in enumerate(result.shape)]
        where[longest] = (where[longest] + shift) % result.shape[longest]
        spots.append(tuple(where))
    return result.at[spots[0]].set(low).at[spots[1]].set(largest)


def block_levels(stream_key, extent, shards, low, largest):
    def one(axis_at, shards_of):
        draws = jax.random.uniform(jax.random.fold_in(jax.random.fold_in(stream_key, 6), axis_at), (shards_of,), jnp.float32, low / len(shards), largest / len(shards))
        return jnp.repeat(jnp.exp(draws), extent[axis_at] // shards_of).reshape((-1,) + (1,) * (len(extent) - axis_at - 1))

    factor_of = one(*shards[0])
    for cut in shards[1:]:
        factor_of = factor_of * one(*cut)
    return factor_of


def centred(stream_key, extent, width, limit, cuts=(), kind=jnp.bfloat16):
    result = jax.random.normal(stream_key, extent, jnp.float32) * width
    if len(cuts) > 0:
        result = block_levels(stream_key, extent, cuts, -0.22, 0.18) * result
    return jnp.clip(result, min=-limit, max=limit).astype(kind)


def setup_inputs(seed: int = 0) -> dict:
    keys = jax.random.split(jax.random.key(seed), 16)
    return {
        "states": centred(keys[0], (SEQ_LEN, D), 1.0, 6.0, ((0, 8),)),
        "inner_weight": centred(keys[1], (D, D_INNER), D ** -0.5, 0.125, ((1, 4),)),
        "gate_weight": draw_gate_weight(jax.random.fold_in(keys[15], 71), 0),
        "state_weight": centred(keys[3], (D, 2 * STATE), D ** -0.5, 0.125),
        "step_weight": centred(keys[4], (D, HEADS), D ** -0.5, 0.125, ((1, 4),)),
        "step_bias": jnp.clip(-4.0 + 2.0 * jax.random.uniform(keys[5], (HEADS,), jnp.float32) ** block_levels(keys[5], (HEADS,), ((0, 4),), -0.2, 0.2), -4.0, -2.0),
        "decay_rate": draw_decay_rate(jax.random.fold_in(keys[15], 71), 0),
        "skip_gain": jnp.clip(0.5 + 1.0 * jax.random.uniform(keys[7], (HEADS,), jnp.float32) ** block_levels(keys[7], (HEADS,), ((0, 4),), -0.2, 0.2), 0.5, 1.5),
        "conv_inner": centred(keys[8], (KCONV, D_INNER), KCONV ** -0.5, 3.0, ((1, 4),), jnp.float32),
        "conv_state": centred(keys[9], (KCONV, 2 * STATE), KCONV ** -0.5, 3.0, (), jnp.float32),
        "norm_gain": jnp.clip(jnp.exp(math.log(2.0) - 1.3862944 * jax.random.uniform(keys[10], (D_INNER,), jnp.float32) ** block_levels(keys[10], (D_INNER,), ((0, 4),), -0.2, 0.2)), 0.5, 2.0),
        "value_weight": centred(keys[11], (D_INNER,), D_INNER ** -0.5, 0.09375, ((0, 4),), jnp.float32),
        "rewards": draw_rewards(jax.random.fold_in(keys[15], 71), 0),
        "done_flags": draw_done_flags(jax.random.fold_in(keys[15], 71), 0),
        "horizon": touch_ends(jax.random.randint(keys[14], (SEQ_LEN,), 1, NSTEP + 1), jax.random.fold_in(keys[14], 1), 1, NSTEP).astype(jnp.int32),
    }


DISCOUNT = 0.99
EXPECTILE = 0.7
EPSILON = 1e-05

def causal_conv(rim_rows, projected, kernel):
    padded = jnp.concatenate([rim_rows.astype(jnp.float32), projected.astype(jnp.float32)], axis=0)
    length = projected.shape[0]
    summed = jnp.zeros(projected.shape, jnp.float32)
    for offset in range(kernel.shape[0]):
        summed = summed + kernel[offset] * padded[offset:offset + length]
    return jax.nn.silu(summed).astype(jnp.bfloat16)

def block_scan(inner, writes, readout, step_size, decay_rate, done_int, running_state):
    precise = lax.Precision.HIGHEST
    inputs = step_size[:, :, None] * inner.astype(jnp.float32)
    local_decay = jnp.cumsum(-decay_rate * step_size, axis=0)
    done_count = jnp.cumsum(done_int)
    done_before = done_count - done_int
    scores = jnp.dot(readout, writes.T, preferred_element_type=jnp.float32)
    positions = jnp.arange(inner.shape[0])
    causal_mask = (positions[:, None] >= positions[None, :]) & (done_before[:, None] == done_before[None, :])
    decay_gap = local_decay[:, None, :] - local_decay[None, :, :]
    weights = scores[:, :, None] * jnp.exp(jnp.where(causal_mask[:, :, None], decay_gap, -jnp.inf))
    block_out = jnp.einsum('tsh,shp->thp', weights, inputs, precision=precise)
    carry_reach = jnp.exp(local_decay) * (done_before == 0)[:, None]
    readout_float = readout.astype(jnp.float32)
    block_out = block_out + carry_reach[:, :, None] * jnp.einsum('tn,hpn->thp', readout_float, running_state, precision=precise)
    tail_weight = jnp.exp(local_decay[-1][None, :] - local_decay) * (done_count[-1] - done_before == 0)[:, None]
    block_state = jnp.einsum('shp,sn->hpn', tail_weight[:, :, None] * inputs, writes.astype(jnp.float32), precision=precise)
    block_decay = jnp.exp(local_decay[-1]) * (done_count[-1] == 0)
    return (block_out, block_decay[:, None, None] * running_state + block_state, block_decay)

def nstep_targets(reward_ext, alive_ext, value_ext, horizon, length):
    targets = jnp.zeros((length,), jnp.float32)
    survive = jnp.ones((length,), jnp.float32)
    for offset in range(NSTEP + 1):
        factor = DISCOUNT ** offset * survive
        targets = targets + jnp.where(offset < horizon, factor * reward_ext[offset:offset + length], 0.0)
        targets = targets + jnp.where(offset == horizon, factor * value_ext[offset:offset + length], 0.0)
        survive = survive * alive_ext[offset:offset + length]
    return targets

def expectile_terms(targets, values):
    residual = targets - values
    return jnp.where(residual < 0, 1.0 - EXPECTILE, EXPECTILE) * residual * residual

def reference(states, inner_weight, gate_weight, state_weight, step_weight, step_bias, decay_rate, skip_gain, conv_inner, conv_state, norm_gain, value_weight, rewards, done_flags, horizon):
    inner_pre = jnp.dot(states, inner_weight, preferred_element_type=jnp.float32).astype(jnp.bfloat16)
    gate_pre = jnp.dot(states, gate_weight, preferred_element_type=jnp.float32).astype(jnp.bfloat16)
    state_pre = jnp.dot(states, state_weight, preferred_element_type=jnp.float32).astype(jnp.bfloat16)
    step_size = jax.nn.softplus(jnp.dot(states, step_weight, preferred_element_type=jnp.float32) + step_bias)
    block_size = math.gcd(SEQ_LEN, 256)
    conv_lag = KCONV - 1

    def advance(carry, block_index):
        running_state, inner_rim, state_rim = carry
        start_row = (block_index * block_size).astype(jnp.int32)
        inner_rows = lax.dynamic_slice_in_dim(inner_pre, start_row, block_size, 0)
        gate_rows = lax.dynamic_slice_in_dim(gate_pre, start_row, block_size, 0)
        state_rows = lax.dynamic_slice_in_dim(state_pre, start_row, block_size, 0)
        step_rows = lax.dynamic_slice_in_dim(step_size, start_row, block_size, 0)
        done_rows = lax.dynamic_slice_in_dim(done_flags, start_row, block_size, 0)
        inner_conv = causal_conv(inner_rim, inner_rows, conv_inner)
        state_conv = causal_conv(state_rim, state_rows, conv_state)
        inner_heads = inner_conv.reshape(block_size, HEADS, HDIM)
        block_out, running_state, unused = block_scan(inner_heads, state_conv[:, :STATE], state_conv[:, STATE:], step_rows, decay_rate, done_rows, running_state)
        mixed_heads = block_out + skip_gain[None, :, None] * inner_heads.astype(jnp.float32)
        gated = mixed_heads.reshape(block_size, D_INNER) * jax.nn.silu(gate_rows.astype(jnp.float32))
        square_sum = lax.optimization_barrier(jnp.sum(gated * gated, axis=1))
        normed = gated * lax.rsqrt(square_sum / D_INNER + EPSILON)[:, None] * norm_gain
        block_values = lax.optimization_barrier(jnp.sum(normed * value_weight, axis=1))
        return ((running_state, inner_rows[block_size - conv_lag:], state_rows[block_size - conv_lag:]), block_values)
    initial = (jnp.zeros((HEADS, HDIM, STATE), jnp.float32), jnp.zeros((conv_lag, D_INNER), jnp.bfloat16), jnp.zeros((conv_lag, 2 * STATE), jnp.bfloat16))
    unused, values = lax.scan(advance, initial, jnp.arange(SEQ_LEN // block_size, dtype=jnp.int32))
    values = values.reshape(SEQ_LEN)
    padding = jnp.zeros((NSTEP,), jnp.float32)
    alive = 1.0 - done_flags.astype(jnp.float32)
    targets = nstep_targets(jnp.concatenate([rewards, padding]), jnp.concatenate([alive, padding]), jnp.concatenate([values, padding]), horizon, SEQ_LEN)
    value_loss = jnp.sum(expectile_terms(targets, values)) / SEQ_LEN
    return (values, targets, value_loss)
```

```python
import functools

import jax
import jax.numpy as jnp
from jax import lax
from jax.experimental import pallas as pl
from jax.experimental.pallas import tpu as pltpu
from jax.sharding import PartitionSpec as P

D_INNER = 4096
NSTEP = 8
DISCOUNT = 0.99
EXPECTILE = 0.7
EPSILON = 1e-05
LANES = 128
HALO = 8
SERIES = 32
RESET = 300.0
VMEM = pl.BlockSpec(memory_space=pltpu.VMEM)
SMEM = pl.BlockSpec(memory_space=pltpu.SMEM)
ANY = pl.BlockSpec(memory_space=pl.ANY)
F32 = jnp.float32
BF16 = jnp.bfloat16


def call(body, outs, ins, scratch=(), flops=0, name=None):
    return pl.pallas_call(
        body,
        out_shape=outs,
        in_specs=ins,
        out_specs=jax.tree.map(lambda _: VMEM, outs),
        scratch_shapes=list(scratch),
        cost_estimate=pl.CostEstimate(flops=flops, transcendentals=0, bytes_accessed=0),
        compiler_params=pltpu.CompilerParams(vmem_limit_bytes=60 * 2**20),
        name=name,
    )


def dot(a, b, dims=((1,), (0,))):
    return lax.dot_general(a, b, (dims, ((), ())), preferred_element_type=F32)


def silu(x):
    return x * jax.nn.sigmoid(x)


def column(scalars, count, shape):
    row = lax.broadcasted_iota(jnp.int32, shape, 0)
    out = jnp.zeros(shape, F32)
    for h in range(count):
        out = jnp.where(row == h, scalars[h], out)
    return out


def project_body(
    bias, decay, done, states, inner_w, state_w, step_w, inner_pre, state_pre, rows, cols, raw
):
    length = states.shape[0]
    heads = bias.shape[0]
    raw[:, :heads] = dot(states[...], step_w[...])
    shape = (heads, length)
    step = raw[...].T[:heads] + column(bias, heads, shape)
    step = jnp.maximum(step, 0.0) + jnp.log1p(jnp.exp(-jnp.abs(step)))
    ended = jnp.broadcast_to(done[...].astype(F32) * RESET, shape)
    total = -column(decay, heads, shape) * step - ended
    lane = lax.broadcasted_iota(jnp.int32, shape, 1)
    stride = 1
    while stride < length:
        total = total + jnp.where(lane >= stride, pltpu.roll(total, stride, 1), 0.0)
        stride *= 2
    reach = total + ended
    last = total[:, length - 1 :]
    rows[0:heads] = reach
    rows[heads : 2 * heads] = step
    rows[2 * heads :] = jnp.broadcast_to(jnp.exp(last), shape)
    tail = jnp.exp(last - reach) * step
    fill = jnp.zeros((LANES - 3 * heads, length), F32)
    cols[...] = jnp.concatenate([tail, reach, jnp.exp(reach), fill], axis=0).T
    width = 256
    for c in range(0, state_w.shape[1], width):
        state_pre[:, c : c + width] = dot(states[...], state_w[:, c : c + width]).astype(BF16)
    for c in range(0, inner_w.shape[1], width):
        inner_pre[:, c : c + width] = dot(states[...], inner_w[:, c : c + width]).astype(BF16)


def conv_body(
    halo,
    inner_w,
    state_w,
    inner_pre,
    state_pre,
    taps_inner,
    taps_state,
    rows,
    cols,
    rewards,
    done,
    horizon,
    inner,
    state,
    message,
    pad,
    weighted,
):
    length = inner_pre.shape[0]
    heads = rows.shape[0] // 3
    shards, depth = message.shape[0], message.shape[1] - 2 * heads - SERIES
    block = LANES

    def convolve(rim, source, taps, target, c, scaled):
        slot = pad.at[c % 2]
        at = slice(c * LANES, (c + 1) * LANES)
        slot[0:HALO] = rim
        slot[HALO:] = source[:, at].astype(F32)
        for r in range(0, length, block):
            out = taps[0:1, at] * slot[r + HALO - 3 : r + HALO - 3 + block]
            for k in range(1, 4):
                out = out + taps[k : k + 1, at] * slot[r + HALO - 3 + k : r + HALO - 3 + k + block]
            out = silu(out).astype(BF16)
            target[r : r + block, at] = out
            if scaled:
                scale = cols[r : r + block, c : c + 1]
                weighted[r : r + block, at] = (out.astype(F32) * scale).astype(BF16)

    rim = dot(halo[...], state_w[...]).astype(BF16).astype(F32)
    for c in range(state_pre.shape[1] // LANES):
        convolve(rim[:, c * LANES : (c + 1) * LANES], state_pre, taps_state, state, c, False)
    writes = state[:, :LANES].astype(F32).T.astype(BF16)
    pair = 2 * LANES
    for c in range(0, heads, 2):
        at = slice(c * LANES, c * LANES + pair)
        rim = dot(halo[...], inner_w[:, at]).astype(BF16).astype(F32)
        convolve(rim[:, :LANES], inner_pre, taps_inner, inner, c, True)
        convolve(rim[:, LANES:], inner_pre, taps_inner, inner, c + 1, True)
        summary = dot(writes, weighted[:, at]).astype(BF16)
        for half in range(2):
            own = summary[:, half * LANES : (half + 1) * LANES]
            first = (c + half) * LANES
            step = min(depth, LANES)
            for q in range(0, LANES, step):
                dest, at_row = divmod(first + q, depth)
                message[dest, at_row : at_row + step] = own[q : q + step]
    total = rows[2 * heads :, 0:LANES]
    high = total.astype(BF16).astype(F32)
    per_row = length // LANES
    split = lambda ref: [ref[:, q * LANES : (q + 1) * LANES].astype(F32) for q in range(per_row)]
    reward = split(rewards)
    first = [r.astype(BF16).astype(F32) for r in reward]
    second = [(r - a).astype(BF16).astype(F32) for r, a in zip(reward, first)]
    third = [r - a - b for r, a, b in zip(reward, first, second)]
    stack = first + second + third + split(done) + split(horizon)
    stack.append(jnp.zeros((SERIES - len(stack), LANES), F32))
    extra = jnp.concatenate([high, total - high] + stack, axis=0).astype(BF16)
    for dest in range(shards):
        message[dest, depth:] = extra


def gate_body(states, gate_w, after, gate):
    del after
    width = 256
    for c in range(0, gate_w.shape[1], width):
        pre = dot(states[...], gate_w[:, c : c + width]).astype(BF16).astype(F32)
        gate[:, c : c + width] = silu(pre)


def scan_body(rank, received, carried):
    shards, depth = carried.shape[0], carried.shape[1]
    heads = shards * depth // LANES
    part = min(depth, LANES)
    row = lax.broadcasted_iota(jnp.int32, (2 * heads, LANES), 0)
    for q in range(0, depth, part):
        head = lax.div(rank[0] * depth + q, LANES)
        state = jnp.zeros((part, LANES), F32)
        for j in range(shards):
            carried[j, q : q + part] = state.astype(BF16)
            both = received[j, depth : depth + 2 * heads].astype(F32)
            keep = (row == head) | (row == head + heads)
            decay = jnp.sum(jnp.where(keep, both, 0.0), axis=0, keepdims=True)
            state = decay * state + received[j, q : q + part].astype(F32)


def shift_time(x, distance):
    lane = lax.broadcasted_iota(jnp.int32, x.shape, 1)
    row = lax.broadcasted_iota(jnp.int32, x.shape, 0)
    count = x.shape[0]
    below = jnp.where(row < count - 1, pltpu.roll(x, count - 1, 0), 0.0)
    moved = jnp.where(lane < distance, below, x)
    return pltpu.roll(moved, LANES - distance, 1)


def inside_body(
    skip, inner, state, rows, cols, received, local, returns, code, scores, reward_s, alive_s, steps_s
):
    length = inner.shape[0]
    heads = rows.shape[0] // 3
    block = LANES
    readout = state[:, LANES:]
    writes = state[:, :LANES]
    scores[...] = dot(readout, writes, ((1,), (1,)))
    below = lax.broadcasted_iota(jnp.int32, (block, block), 0) >= lax.broadcasted_iota(
        jnp.int32, (block, block), 1
    )
    for h in range(heads):
        at = slice(h * LANES, (h + 1) * LANES)
        for r in range(0, length, block):
            here = jnp.broadcast_to(cols[r : r + block, heads + h : heads + h + 1], (block, LANES))
            pieces = []
            for s in range(0, r + block, block):
                gap = here - rows[h : h + 1, s : s + block]
                if s == r:
                    gap = jnp.where(below, gap, -jnp.inf)
                weight = scores[r : r + block, s : s + block] * rows[heads + h : heads + h + 1, s : s + block]
                pieces.append((jnp.exp(gap) * weight).astype(BF16))
            weights = jnp.concatenate(pieces, axis=1)
            out = dot(weights, inner[0 : r + block, at])
            local[r : r + block, at] = out + skip[h] * inner[r : r + block, at].astype(F32)
    shards = received.shape[0]
    series = received.shape[1] - SERIES
    per = length // LANES
    for j in range(shards):
        extra = received[j, series:].astype(F32)
        to = slice(j * per, (j + 1) * per)
        reward_s[to] = extra[0:per] + extra[per : 2 * per] + extra[2 * per : 3 * per]
        alive_s[to] = 1.0 - extra[3 * per : 4 * per]
        steps_s[to] = extra[4 * per : 5 * per]
    reward, alive, steps = reward_s[...], alive_s[...], steps_s[...]
    gained = jnp.zeros(reward.shape, F32)
    survive = jnp.ones(reward.shape, F32)
    reached = jnp.zeros(reward.shape, F32)
    for offset in range(NSTEP + 1):
        ahead = shift_time(reward, offset) if offset else reward
        gained = gained + jnp.where(offset < steps, DISCOUNT**offset * survive * ahead, 0.0)
        reached = jnp.where(offset == steps, survive * offset, reached)
        if offset < NSTEP:
            survive = survive * (shift_time(alive, offset) if offset else alive)
    returns[...] = gained
    code[...] = reached


def finish_body(state, carried, local, gate, cols, norm_gain, value_weight, message):
    length = state.shape[0]
    heads = carried.shape[0] // LANES
    block = LANES
    weight = norm_gain[...] * value_weight[...]
    squares, sums = [], []
    for r in range(0, length, block):
        readout = state[r : r + block, LANES:]
        square = jnp.zeros((block, LANES), F32)
        total = jnp.zeros((block, LANES), F32)
        for c in range(0, heads, 2):
            both = jnp.concatenate(
                [carried[(c + i) * LANES : (c + i + 1) * LANES] for i in range(2)], axis=1
            )
            fix = dot(readout, both)
            for i in range(2):
                h = c + i
                at = slice(h * LANES, (h + 1) * LANES)
                reach = cols[r : r + block, 2 * heads + h : 2 * heads + h + 1]
                mixed = local[r : r + block, at] + reach * fix[:, i * LANES : (i + 1) * LANES]
                gated = mixed * gate[r : r + block, at]
                square = square + gated * gated
                total = total + gated * weight[:, at]
        squares.append(jnp.sum(square.T, axis=0, keepdims=True))
        sums.append(jnp.sum(total.T, axis=0, keepdims=True))
    tile = jnp.concatenate(squares + sums, axis=0)
    for dest in range(message.shape[0]):
        message[dest] = tile


def loss_body(rank, received, returns, code, values, targets, loss, values_s, targets_s):
    devices, double, _ = received.shape
    per = double // 2
    total_rows = returns.shape[0]
    shards = total_rows // per
    group = devices // shards
    for j in range(shards):
        tile = received[group * j]
        for g in range(1, group):
            tile = tile + received[group * j + g]
        values_s[per * j : per * (j + 1)] = tile[per:] * lax.rsqrt(tile[:per] / D_INNER + EPSILON)
    value = values_s[...]
    reached = code[...]
    target = returns[...]
    for offset in range(1, NSTEP + 1):
        ahead = shift_time(value, offset)
        target = target + jnp.where(reached == offset, DISCOUNT**offset * ahead, 0.0)
    targets_s[...] = target
    residual = target - value
    terms = jnp.where(residual < 0, 1.0 - EXPECTILE, EXPECTILE) * residual * residual
    loss[...] = jnp.sum(jnp.sum(terms, axis=0, keepdims=True), axis=1, keepdims=True) / (
        total_rows * LANES
    )
    own = pl.ds(rank[0] * per, per)
    values[...] = values_s[own]
    targets[...] = targets_s[own]


def per_device(
    states,
    inner_weight,
    gate_weight,
    state_weight,
    step_weight,
    step_bias,
    decay_rate,
    skip_gain,
    conv_inner,
    conv_state,
    norm_gain,
    value_weight,
    rewards,
    done_flags,
    horizon,
):
    length = states.shape[0]
    heads = step_bias.shape[0]
    inner_width = inner_weight.shape[1]
    state_width = state_weight.shape[1]
    shards = lax.axis_size("seq")
    devices = shards * lax.axis_size("head")
    depth = heads * LANES // shards
    per = length // LANES
    rank = lax.axis_index("seq").astype(jnp.int32).reshape(1)
    shape = jax.ShapeDtypeStruct
    done_row = done_flags.reshape(1, length)

    halo = lax.ppermute(
        states[length - HALO :], "seq", [(i, i + 1) for i in range(shards - 1)]
    )
    inner_pre, state_pre, rows, cols = call(
        project_body,
        [
            shape((length, inner_width), BF16),
            shape((length, state_width), BF16),
            shape((3 * heads, length), F32),
            shape((length, LANES), F32),
        ],
        [SMEM, SMEM] + [VMEM] * 5,
        [pltpu.VMEM((length, LANES), F32)],
        flops=2 * length * states.shape[1] * (inner_width + state_width),
        name="project",
    )(step_bias, decay_rate, done_row, states, inner_weight, state_weight, step_weight)
    inner, state, message = call(
        conv_body,
        [
            shape((length, inner_width), BF16),
            shape((length, state_width), BF16),
            shape((shards, depth + 2 * heads + SERIES, LANES), BF16),
        ],
        [VMEM] * 12,
        [pltpu.VMEM((2, length + HALO, LANES), F32), pltpu.VMEM((length, inner_width), BF16)],
        flops=length * inner_width * 600,
        name="conv",
    )(
        halo,
        inner_weight,
        state_weight,
        inner_pre,
        state_pre,
        conv_inner,
        conv_state,
        rows,
        cols,
        rewards.reshape(1, length),
        done_row,
        horizon.reshape(1, length),
    )
    received = lax.all_to_all(message, "seq", 0, 0, tiled=True)
    gate = call(
        gate_body,
        shape((length, inner_width), F32),
        [VMEM, VMEM, ANY],
        flops=2 * length * states.shape[1] * inner_width,
        name="gate",
    )(states, gate_weight, message)
    carried = call(
        scan_body,
        shape((shards, depth, LANES), BF16),
        [SMEM, VMEM],
        name="scan",
    )(rank, received)
    entered = lax.all_to_all(carried, "seq", 0, 0, tiled=True).reshape(heads * LANES, LANES)
    trajectory = shape((shards * per, LANES), F32)
    local, returns, code = call(
        inside_body,
        [shape((length, inner_width), F32), trajectory, trajectory],
        [SMEM] + [VMEM] * 5,
        [pltpu.VMEM((length, length), F32)] + [pltpu.VMEM((shards * per, LANES), F32)] * 3,
        flops=length * length * inner_width * 4,
        name="inside",
    )(skip_gain, inner, state, rows, cols, received)
    parts = call(
        finish_body,
        shape((devices, 2 * per, LANES), F32),
        [VMEM] * 7,
        flops=length * inner_width * 300,
        name="finish",
    )(
        state,
        entered,
        local,
        gate,
        cols,
        norm_gain.reshape(1, inner_width),
        value_weight.reshape(1, inner_width),
    )
    everything = lax.all_to_all(parts, ("seq", "head"), 0, 0, tiled=True)
    own = shape((per, LANES), F32)
    values, targets, value_loss = call(
        loss_body,
        [own, own, shape((1, 1), F32)],
        [SMEM] + [VMEM] * 3,
        [pltpu.VMEM((shards * per, LANES), F32)] * 2,
        name="loss",
    )(rank, everything, returns, code)
    return values.reshape(length), targets.reshape(length), value_loss.reshape(())


def solution(mesh):
    placed = (
        P("seq", None),
        P(None, "head"),
        P(None, "head"),
        P(),
        P(None, "head"),
        P("head"),
        P("head"),
        P("head"),
        P(None, "head"),
        P(),
        P("head"),
        P("head"),
        P("seq"),
        P("seq"),
        P("seq"),
    )
    return jax.shard_map(
        per_device, mesh=mesh, in_specs=placed, out_specs=(P("seq"), P("seq"), P()), check_vma=False
    )
```

```python
import functools

import jax
import jax.numpy as jnp
from jax import lax
from jax.experimental import pallas as pl
from jax.experimental.pallas import tpu as pltpu
from jax.sharding import PartitionSpec as P

D_INNER = 4096
NSTEP = 8
DISCOUNT = 0.99
EXPECTILE = 0.7
EPSILON = 1e-05
LANES = 128
HALO = 8
RESET = 300.0
VMEM = pl.BlockSpec(memory_space=pltpu.VMEM)
SMEM = pl.BlockSpec(memory_space=pltpu.SMEM)
ANY = pl.BlockSpec(memory_space=pl.ANY)
HBM = pl.BlockSpec(memory_space=pltpu.HBM)
F32 = jnp.float32
BF16 = jnp.bfloat16


def call(body, outs, ins, scratch=(), flops=0, moved=0, name=None, limit=10):
    return pl.pallas_call(
        body,
        out_shape=outs,
        in_specs=ins,
        out_specs=jax.tree.map(lambda _: VMEM, outs),
        scratch_shapes=list(scratch),
        cost_estimate=pl.CostEstimate(flops=flops, transcendentals=0, bytes_accessed=moved),
        compiler_params=pltpu.CompilerParams(vmem_limit_bytes=limit * 2**20),
        name=name,
    )


def in_hbm(x):
    return pltpu.with_memory_space_constraint(x, pltpu.HBM)


def dot(a, b, dims=((1,), (0,))):
    return lax.dot_general(a, b, (dims, ((), ())), preferred_element_type=F32)


def silu(x):
    return x * jax.nn.sigmoid(x)


def column(scalars, count, shape):
    row = lax.broadcasted_iota(jnp.int32, shape, 0)
    out = jnp.zeros(shape, F32)
    for h in range(count):
        out = jnp.where(row == h, scalars[h], out)
    return out


def entry_body(
    bias_hbm,
    decay_hbm,
    done_hbm,
    states_hbm,
    state_hbm,
    step_hbm,
    states,
    state_w,
    state_pre,
    rows,
    cols,
    edge,
    step_w,
    done,
    bias,
    decay,
    arrived,
):
    length = states.shape[0]
    heads = bias.shape[0]
    pairs = [(states_hbm, states), (step_hbm, step_w), (done_hbm, done)]
    pairs += [(bias_hbm, bias), (decay_hbm, decay), (state_hbm, state_w)]
    copies = [pltpu.make_async_copy(*pair, arrived.at[i]) for i, pair in enumerate(pairs)]
    for copy in copies:
        copy.start()
    for copy in copies:
        copy.wait()
    edge[...] = states[length - HALO :]
    step_rows(bias, decay, done, states, step_w, rows, cols, heads, length)
    width = 2 * LANES
    for c in range(0, state_w.shape[1], width):
        state_pre[:, c : c + width] = dot(states[...], state_w[:, c : c + width]).astype(BF16)


def project_body(states, inner_w, inner_pre):
    width = 2 * LANES
    for c in range(0, inner_w.shape[1], width):
        inner_pre[:, c : c + width] = dot(states[...], inner_w[:, c : c + width]).astype(BF16)


def step_rows(bias, decay, done, states, step_w, rows, cols, heads, length):
    shape = (heads, length)
    step = dot(step_w[...], states[...], ((1,), (1,))) + column(bias, heads, shape)
    step = jnp.maximum(step, 0.0) + jnp.log1p(jnp.exp(-jnp.abs(step)))
    ended = jnp.broadcast_to(done[...].astype(F32) * RESET, shape)
    total = -column(decay, heads, shape) * step - ended
    lane = lax.broadcasted_iota(jnp.int32, shape, 1)
    stride = 1
    while stride < length:
        total = total + jnp.where(lane >= stride, pltpu.roll(total, stride, 1), 0.0)
        stride *= 2
    reach = total + ended
    last = total[:, length - 1 :]
    rows[0:heads] = reach
    rows[heads : 2 * heads] = step
    rows[2 * heads :] = jnp.broadcast_to(jnp.exp(last), shape)
    tail = jnp.exp(last - reach) * step
    fill = jnp.zeros((LANES - 3 * heads, length), F32)
    cols[...] = jnp.concatenate([tail, reach, jnp.exp(reach), fill], axis=0).T


def conv_body(
    halo,
    inner_w,
    state_w,
    inner_pre,
    state_pre,
    taps_inner,
    taps_state,
    rows,
    cols,
    rewards,
    done,
    horizon,
    inner,
    state,
    message,
    pad,
    weighted,
):
    length = inner_pre.shape[0]
    heads = rows.shape[0] // 3
    shards = message.shape[0]
    depth = heads * LANES // shards
    block = LANES

    def convolve(rim, source, taps, target, c, scaled):
        slot = pad.at[c % 2]
        at = slice(c * LANES, (c + 1) * LANES)
        slot[0:HALO] = rim
        slot[HALO:] = source[:, at].astype(F32)
        for r in range(0, length, block):
            out = taps[0:1, at] * slot[r + HALO - 3 : r + HALO - 3 + block]
            for k in range(1, 4):
                out = out + taps[k : k + 1, at] * slot[r + HALO - 3 + k : r + HALO - 3 + k + block]
            out = silu(out).astype(BF16)
            target[r : r + block, at] = out
            if scaled:
                scale = cols[r : r + block, c : c + 1]
                weighted[r : r + block, at] = (out.astype(F32) * scale).astype(BF16)

    rim = dot(halo[...], state_w[...]).astype(BF16).astype(F32)
    for c in range(state_pre.shape[1] // LANES):
        convolve(rim[:, c * LANES : (c + 1) * LANES], state_pre, taps_state, state, c, False)
    writes = state[:, :LANES].astype(F32).T.astype(BF16)
    pair = 2 * LANES
    for c in range(0, heads, 2):
        at = slice(c * LANES, c * LANES + pair)
        rim = dot(halo[...], inner_w[:, at]).astype(BF16).astype(F32)
        convolve(rim[:, :LANES], inner_pre, taps_inner, inner, c, True)
        convolve(rim[:, LANES:], inner_pre, taps_inner, inner, c + 1, True)
        summary = dot(writes, weighted[:, at]).astype(BF16)
        for half in range(2):
            own = summary[:, half * LANES : (half + 1) * LANES]
            first = (c + half) * LANES
            step = min(depth, LANES)
            for q in range(0, LANES, step):
                dest, at_row = divmod(first + q, depth)
                message[dest, at_row : at_row + step] = own[q : q + step]
    total = rows[2 * heads :, 0:LANES]
    high = total.astype(BF16).astype(F32)
    low = total - high
    per = length // LANES
    reward = lane_rows(rewards, per)
    first = reward.astype(BF16).astype(F32)
    second = (reward - first).astype(BF16).astype(F32)
    series = [first, second, reward - first - second, lane_rows(done, per), lane_rows(horizon, per)]
    held = max(1, depth // LANES)
    spare = message.shape[1] - depth - 5 * per - 2 * held
    if spare:
        series.append(jnp.zeros((spare, LANES), F32))
    for dest in range(shards):
        head = dest * depth // LANES
        decays = [high[head : head + held], low[head : head + held]]
        message[dest, depth:] = jnp.concatenate(series + decays, axis=0).astype(BF16)


def lane_rows(ref, count):
    pieces = [ref[:, q * LANES : (q + 1) * LANES].astype(F32) for q in range(count)]
    return jnp.concatenate(pieces, axis=0)


def gate_body(
    rank,
    states_hbm,
    gate_hbm,
    received,
    after,
    gate,
    returns,
    code,
    states,
    gate_w,
    reward_s,
    alive_s,
    steps_s,
    arrived,
):
    del rank
    pairs = [(gate_hbm, gate_w), (states_hbm, states)]
    copies = [pltpu.make_async_copy(*pair, arrived.at[i]) for i, pair in enumerate(pairs)]
    for copy in copies:
        copy.start()
    depth = after.shape[1]
    series(received, depth, states.shape[0] // LANES, returns, code, reward_s, alive_s, steps_s)
    for copy in copies:
        copy.wait()
    width = 2 * LANES
    for c in range(0, gate_w.shape[1], width):
        pre = dot(states[...], gate_w[:, c : c + width]).astype(BF16).astype(F32)
        gate[:, c : c + width] = silu(pre).astype(gate.dtype)


def series(received, depth, per, returns, code, reward_s, alive_s, steps_s):
    shards = received.shape[0]
    for j in range(shards):
        extra = received[j, depth:].astype(F32)
        to = slice(j * per, (j + 1) * per)
        reward_s[to] = extra[0:per] + extra[per : 2 * per] + extra[2 * per : 3 * per]
        alive_s[to] = 1.0 - extra[3 * per : 4 * per]
        steps_s[to] = extra[4 * per : 5 * per]
    reward, alive, steps = reward_s[...], alive_s[...], steps_s[...]
    gained = jnp.zeros(reward.shape, F32)
    survive = jnp.ones(reward.shape, F32)
    reached = jnp.zeros(reward.shape, F32)
    for offset in range(NSTEP + 1):
        ahead = shift_time(reward, offset) if offset else reward
        gained = gained + jnp.where(offset < steps, DISCOUNT**offset * survive * ahead, 0.0)
        reached = jnp.where(offset == steps, survive * offset, reached)
        if offset < NSTEP:
            survive = survive * (shift_time(alive, offset) if offset else alive)
    returns[...] = gained
    code[...] = reached


def scan_body(received, after, carried):
    del after
    shards, depth = carried.shape[0], carried.shape[1]
    held = max(1, depth // LANES)
    part = min(depth, LANES)
    end = received.shape[1]
    for q in range(held):
        state = jnp.zeros((part, LANES), F32)
        for j in range(shards):
            carried[j, q * part : (q + 1) * part] = state.astype(BF16)
            both = received[j, depth:end].astype(F32)
            high = both[end - depth - 2 * held + q : end - depth - 2 * held + q + 1]
            low = both[end - depth - held + q : end - depth - held + q + 1]
            state = (high + low) * state + received[j, q * part : (q + 1) * part].astype(F32)


def shift_time(x, distance):
    lane = lax.broadcasted_iota(jnp.int32, x.shape, 1)
    row = lax.broadcasted_iota(jnp.int32, x.shape, 0)
    count = x.shape[0]
    below = jnp.where(row < count - 1, pltpu.roll(x, count - 1, 0), 0.0)
    moved = jnp.where(lane < distance, below, x)
    return pltpu.roll(moved, LANES - distance, 1)


def inside_body(
    skip, inner, state, rows, cols, local, scores
):
    length = inner.shape[0]
    heads = rows.shape[0] // 3
    block = LANES
    readout = state[:, LANES:]
    writes = state[:, :LANES]
    scores[...] = dot(readout, writes, ((1,), (1,)))
    below = lax.broadcasted_iota(jnp.int32, (block, block), 0) >= lax.broadcasted_iota(
        jnp.int32, (block, block), 1
    )
    for h in range(heads):
        at = slice(h * LANES, (h + 1) * LANES)
        for r in range(0, length, block):
            here = jnp.broadcast_to(cols[r : r + block, heads + h : heads + h + 1], (block, LANES))
            pieces = []
            for s in range(0, r + block, block):
                gap = here - rows[h : h + 1, s : s + block]
                if s == r:
                    gap = jnp.where(below, gap, -jnp.inf)
                weight = scores[r : r + block, s : s + block] * rows[heads + h : heads + h + 1, s : s + block]
                pieces.append((jnp.exp(gap) * weight).astype(BF16))
            weights = jnp.concatenate(pieces, axis=1)
            out = dot(weights, inner[0 : r + block, at])
            out = out + skip[h] * inner[r : r + block, at].astype(F32)
            local[r : r + block, at] = out.astype(local.dtype)


def finish_body(state, carried, local, gate, cols, norm_gain, value_weight, message):
    length = state.shape[0]
    heads = carried.shape[0] // LANES
    block = LANES
    weight = norm_gain[...] * value_weight[...]
    squares, sums = [], []
    for r in range(0, length, block):
        readout = state[r : r + block, LANES:]
        square = jnp.zeros((block, LANES), F32)
        total = jnp.zeros((block, LANES), F32)
        for c in range(0, heads, 2):
            both = jnp.concatenate(
                [carried[(c + i) * LANES : (c + i + 1) * LANES] for i in range(2)], axis=1
            )
            fix = dot(readout, both)
            for i in range(2):
                h = c + i
                at = slice(h * LANES, (h + 1) * LANES)
                reach = cols[r : r + block, 2 * heads + h : 2 * heads + h + 1]
                mixed = local[r : r + block, at].astype(F32) + reach * fix[:, i * LANES : (i + 1) * LANES]
                gated = mixed * gate[r : r + block, at].astype(F32)
                square = square + gated * gated
                total = total + gated * weight[:, at]
        squares.append(jnp.sum(square.T, axis=0, keepdims=True))
        sums.append(jnp.sum(total.T, axis=0, keepdims=True))
    tile = jnp.concatenate(squares + sums, axis=0)
    for dest in range(message.shape[0]):
        message[dest] = tile


def loss_body(rank, received, returns, code, values, targets, loss, values_s, targets_s):
    devices, double, _ = received.shape
    per = double // 2
    total_rows = returns.shape[0]
    shards = total_rows // per
    group = devices // shards
    for j in range(shards):
        tile = received[group * j]
        for g in range(1, group):
            tile = tile + received[group * j + g]
        values_s[per * j : per * (j + 1)] = tile[per:] * lax.rsqrt(tile[:per] / D_INNER + EPSILON)
    value = values_s[...]
    reached = code[...]
    target = returns[...]
    for offset in range(1, NSTEP + 1):
        ahead = shift_time(value, offset)
        target = target + jnp.where(reached == offset, DISCOUNT**offset * ahead, 0.0)
    targets_s[...] = target
    residual = target - value
    terms = jnp.where(residual < 0, 1.0 - EXPECTILE, EXPECTILE) * residual * residual
    loss[...] = jnp.sum(jnp.sum(terms, axis=0, keepdims=True), axis=1, keepdims=True) / (
        total_rows * LANES
    )
    own = pl.ds(rank[0] * per, per)
    values[...] = values_s[own]
    targets[...] = targets_s[own]


def per_device(
    states,
    inner_weight,
    gate_weight,
    state_weight,
    step_weight,
    step_bias,
    decay_rate,
    skip_gain,
    conv_inner,
    conv_state,
    norm_gain,
    value_weight,
    rewards,
    done_flags,
    horizon,
):
    length = states.shape[0]
    heads = step_bias.shape[0]
    inner_width = inner_weight.shape[1]
    state_width = state_weight.shape[1]
    shards = lax.axis_size("seq")
    devices = shards * lax.axis_size("head")
    depth = heads * LANES // shards
    per = length // LANES
    packed = -(-(5 * per + 2 * max(1, depth // LANES)) // 8) * 8
    rank = lax.axis_index("seq").astype(jnp.int32).reshape(1)
    shape = jax.ShapeDtypeStruct
    done_row = done_flags.reshape(1, length)

    states_near, state_weight, state_pre, rows, cols, edge = call(
        entry_body,
        [
            shape(states.shape, BF16),
            shape(state_weight.shape, BF16),
            shape((length, state_width), BF16),
            shape((3 * heads, length), F32),
            shape((length, LANES), F32),
            shape((HALO, states.shape[1]), BF16),
        ],
        [HBM] * 6,
        [
            pltpu.VMEM(step_weight.shape[::-1], BF16),
            pltpu.VMEM((1, length), jnp.int32),
            pltpu.SMEM((heads,), F32),
            pltpu.SMEM((heads,), F32),
            pltpu.SemaphoreType.DMA((6,)),
        ],
        flops=2 * length * states.shape[1] * inner_width,
        moved=4 * states.size,
        name="entry",
    )(
        in_hbm(step_bias),
        in_hbm(decay_rate),
        in_hbm(done_row),
        in_hbm(states),
        in_hbm(state_weight),
        in_hbm(step_weight.T),
    )
    halo = lax.ppermute(edge, "seq", [(i, i + 1) for i in range(shards - 1)])
    inner_pre = call(
        project_body,
        shape((length, inner_width), BF16),
        [VMEM, VMEM],
        flops=2 * length * states.shape[1] * inner_width,
        name="project",
    )(states_near, inner_weight)
    inner, state, message = call(
        conv_body,
        [
            shape((length, inner_width), BF16),
            shape((length, state_width), BF16),
            shape((shards, depth + packed, LANES), BF16),
        ],
        [VMEM] * 12,
        [pltpu.VMEM((2, length + HALO, LANES), F32), pltpu.VMEM((length, inner_width), BF16)],
        flops=length * inner_width * 600,
        name="conv",
    )(
        halo,
        inner_weight,
        state_weight,
        inner_pre,
        state_pre,
        conv_inner,
        conv_state,
        rows,
        cols,
        rewards.reshape(1, length),
        done_row,
        horizon.reshape(1, length),
    )
    received = lax.all_to_all(message, "seq", 0, 0, tiled=True)
    local = call(
        inside_body,
        shape((length, inner_width), BF16),
        [SMEM] + [VMEM] * 4,
        [pltpu.VMEM((length, length), F32)],
        flops=length * length * inner_width * 4,
        name="inside",
    )(skip_gain, inner, state, rows, cols)
    carried = call(
        scan_body,
        shape((shards, depth, LANES), BF16),
        [VMEM, ANY],
        name="scan",
    )(received, local)
    entered = lax.all_to_all(carried, "seq", 0, 0, tiled=True).reshape(heads * LANES, LANES)
    trajectory = shape((shards * per, LANES), F32)
    gate, returns, code = call(
        gate_body,
        [shape((length, inner_width), BF16), trajectory, trajectory],
        [SMEM, HBM, HBM, VMEM, ANY],
        [pltpu.VMEM(states.shape, BF16), pltpu.VMEM(gate_weight.shape, BF16)]
        + [pltpu.VMEM((shards * per, LANES), F32)] * 3
        + [pltpu.SemaphoreType.DMA((2,))],
        flops=2 * length * states.shape[1] * inner_width,
        name="gate",
    )(rank, in_hbm(states), in_hbm(gate_weight), received, carried)
    parts = call(
        finish_body,
        shape((devices, 2 * per, LANES), F32),
        [VMEM] * 7,
        flops=length * inner_width * 300,
        name="finish",
    )(
        state,
        entered,
        local,
        gate,
        cols,
        norm_gain.reshape(1, inner_width),
        value_weight.reshape(1, inner_width),
    )
    everything = lax.all_to_all(parts, ("seq", "head"), 0, 0, tiled=True)
    own = shape((per, LANES), F32)
    values, targets, value_loss = call(
        loss_body,
        [own, own, shape((1, 1), F32)],
        [SMEM] + [VMEM] * 3,
        [pltpu.VMEM((shards * per, LANES), F32)] * 2,
        name="loss",
    )(rank, everything, returns, code)
    return values.reshape(length), targets.reshape(length), value_loss.reshape(())


def solution(mesh):
    placed = (
        P("seq", None),
        P(None, "head"),
        P(None, "head"),
        P(),
        P(None, "head"),
        P("head"),
        P("head"),
        P("head"),
        P(None, "head"),
        P(),
        P("head"),
        P("head"),
        P("seq"),
        P("seq"),
        P("seq"),
    )
    return jax.shard_map(
        per_device, mesh=mesh, in_specs=placed, out_specs=(P("seq"), P("seq"), P()), check_vma=False
    )
```

```python
import functools

import jax
import jax.numpy as jnp
from jax import lax
from jax.experimental import pallas as pl
from jax.experimental.pallas import tpu as pltpu
from jax.sharding import PartitionSpec as P

D_INNER = 4096
NSTEP = 8
DISCOUNT = 0.99
EXPECTILE = 0.7
EPSILON = 1e-05
LANES = 128
HALO = 8
CONV_ROWS = 32
RESET = 300.0
VMEM = pl.BlockSpec(memory_space=pltpu.VMEM)
SMEM = pl.BlockSpec(memory_space=pltpu.SMEM)
ANY = pl.BlockSpec(memory_space=pl.ANY)
HBM = pl.BlockSpec(memory_space=pltpu.HBM)
F32 = jnp.float32
BF16 = jnp.bfloat16


def call(body, outs, ins, scratch=(), flops=0, moved=0, name=None, limit=10):
    return pl.pallas_call(
        body,
        out_shape=outs,
        in_specs=ins,
        out_specs=jax.tree.map(lambda _: VMEM, outs),
        scratch_shapes=list(scratch),
        cost_estimate=pl.CostEstimate(flops=flops, transcendentals=0, bytes_accessed=moved),
        compiler_params=pltpu.CompilerParams(vmem_limit_bytes=limit * 2**20),
        name=name,
    )


def in_hbm(x):
    return pltpu.with_memory_space_constraint(x, pltpu.HBM)


def dot(a, b, dims=((1,), (0,))):
    return lax.dot_general(a, b, (dims, ((), ())), preferred_element_type=F32)


def silu(x):
    return x * jax.nn.sigmoid(x)


def column(scalars, count, shape):
    row = lax.broadcasted_iota(jnp.int32, shape, 0)
    out = jnp.zeros(shape, F32)
    for h in range(count):
        out = jnp.where(row == h, scalars[h], out)
    return out


def edge_body(states_hbm, edge, arrived):
    rows = pl.ds(states_hbm.shape[0] - HALO, HALO)
    copy = pltpu.make_async_copy(states_hbm.at[rows], edge, arrived)
    copy.start()
    copy.wait()


def project_body(
    bias, decay, done, states, step_w, state_w, inner_w, inner_pre, state_pre, rows, cols
):
    length = states.shape[0]
    heads = bias.shape[0]
    width = 2 * LANES
    for c in range(0, state_w.shape[1], width):
        state_pre[:, c : c + width] = dot(states[...], state_w[:, c : c + width]).astype(BF16)
    for c in range(0, inner_w.shape[1], width):
        if c == width:
            step_rows(bias, decay, done, states, step_w, rows, cols, heads, length)
        inner_pre[:, c : c + width] = dot(states[...], inner_w[:, c : c + width]).astype(BF16)


def step_rows(bias, decay, done, states, step_w, rows, cols, heads, length):
    shape = (heads, length)
    step = dot(step_w[...], states[...], ((1,), (1,))) + column(bias, heads, shape)
    step = jnp.maximum(step, 0.0) + jnp.log1p(jnp.exp(-jnp.abs(step)))
    ended = jnp.broadcast_to(done[...].astype(F32) * RESET, shape)
    total = -column(decay, heads, shape) * step - ended
    lane = lax.broadcasted_iota(jnp.int32, shape, 1)
    stride = 1
    while stride < length:
        total = total + jnp.where(lane >= stride, pltpu.roll(total, stride, 1), 0.0)
        stride *= 2
    reach = total + ended
    last = total[:, length - 1 :]
    rows[0:heads] = reach
    rows[heads : 2 * heads] = step
    rows[2 * heads :] = jnp.broadcast_to(jnp.exp(last), shape)
    tail = jnp.exp(last - reach) * step
    fill = jnp.zeros((LANES - 3 * heads, length), F32)
    cols[...] = jnp.concatenate([tail, reach, jnp.exp(reach), fill], axis=0).T


def conv_body(
    halo,
    inner_w,
    state_w,
    inner_pre,
    state_pre,
    taps_inner,
    taps_state,
    rows,
    cols,
    rewards,
    done,
    horizon,
    inner,
    state,
    message,
    pad,
    weighted,
):
    length = inner_pre.shape[0]
    heads = rows.shape[0] // 3
    shards = message.shape[0]
    depth = heads * LANES // shards
    block = CONV_ROWS

    def convolve(rim, source, taps, target, c, scaled):
        slot = pad.at[c % 2]
        at = slice(c * LANES, (c + 1) * LANES)
        slot[0:HALO] = rim
        for r in range(0, length, block):
            here = source[r : r + block, at].astype(F32)
            slot[r + HALO : r + HALO + block] = here
            out = taps[3:4, at] * here
            for k in range(3):
                out = out + taps[k : k + 1, at] * slot[r + HALO - 3 + k : r + HALO - 3 + k + block]
            out = silu(out).astype(BF16)
            target[r : r + block, at] = out
            if scaled:
                scale = cols[r : r + block, c : c + 1]
                weighted[r : r + block, at] = (out.astype(F32) * scale).astype(BF16)

    rim = dot(halo[...], state_w[...]).astype(BF16).astype(F32)
    for c in range(state_pre.shape[1] // LANES):
        convolve(rim[:, c * LANES : (c + 1) * LANES], state_pre, taps_state, state, c, False)
    writes = state[:, :LANES].astype(F32).T.astype(BF16)
    pair = 2 * LANES
    for c in range(0, heads, 2):
        at = slice(c * LANES, c * LANES + pair)
        rim = dot(halo[...], inner_w[:, at]).astype(BF16).astype(F32)
        convolve(rim[:, :LANES], inner_pre, taps_inner, inner, c, True)
        convolve(rim[:, LANES:], inner_pre, taps_inner, inner, c + 1, True)
        summary = dot(writes, weighted[:, at]).astype(BF16)
        for half in range(2):
            own = summary[:, half * LANES : (half + 1) * LANES]
            first = (c + half) * LANES
            step = min(depth, LANES)
            for q in range(0, LANES, step):
                dest, at_row = divmod(first + q, depth)
                message[dest, at_row : at_row + step] = own[q : q + step]
    total = rows[2 * heads :, 0:LANES]
    high = total.astype(BF16).astype(F32)
    low = total - high
    per = length // LANES
    reward = lane_rows(rewards, per)
    first = reward.astype(BF16).astype(F32)
    second = (reward - first).astype(BF16).astype(F32)
    series = [first, second, reward - first - second, lane_rows(done, per), lane_rows(horizon, per)]
    held = max(1, depth // LANES)
    spare = message.shape[1] - depth - 5 * per - 2 * held
    if spare:
        series.append(jnp.zeros((spare, LANES), F32))
    for dest in range(shards):
        head = dest * depth // LANES
        decays = [high[head : head + held], low[head : head + held]]
        message[dest, depth:] = jnp.concatenate(series + decays, axis=0).astype(BF16)


def lane_rows(ref, count):
    pieces = [ref[:, q * LANES : (q + 1) * LANES].astype(F32) for q in range(count)]
    return jnp.concatenate(pieces, axis=0)


def gate_body(
    rank,
    states_hbm,
    gate_hbm,
    received,
    after,
    gate,
    returns,
    code,
    states,
    gate_w,
    reward_s,
    alive_s,
    steps_s,
    arrived,
):
    del rank
    pairs = [(gate_hbm, gate_w), (states_hbm, states)]
    copies = [pltpu.make_async_copy(*pair, arrived.at[i]) for i, pair in enumerate(pairs)]
    for copy in copies:
        copy.start()
    depth = after.shape[1]
    series(received, depth, states.shape[0] // LANES, returns, code, reward_s, alive_s, steps_s)
    for copy in copies:
        copy.wait()
    width = 2 * LANES
    for c in range(0, gate_w.shape[1], width):
        pre = dot(states[...], gate_w[:, c : c + width]).astype(BF16).astype(F32)
        gate[:, c : c + width] = silu(pre).astype(gate.dtype)


def series(received, depth, per, returns, code, reward_s, alive_s, steps_s):
    shards = received.shape[0]
    for j in range(shards):
        extra = received[j, depth:].astype(F32)
        to = slice(j * per, (j + 1) * per)
        reward_s[to] = extra[0:per] + extra[per : 2 * per] + extra[2 * per : 3 * per]
        alive_s[to] = 1.0 - extra[3 * per : 4 * per]
        steps_s[to] = extra[4 * per : 5 * per]
    reward, alive, steps = reward_s[...], alive_s[...], steps_s[...]
    gained = jnp.zeros(reward.shape, F32)
    survive = jnp.ones(reward.shape, F32)
    reached = jnp.zeros(reward.shape, F32)
    for offset in range(NSTEP + 1):
        ahead = shift_time(reward, offset) if offset else reward
        gained = gained + jnp.where(offset < steps, DISCOUNT**offset * survive * ahead, 0.0)
        reached = jnp.where(offset == steps, survive * offset, reached)
        if offset < NSTEP:
            survive = survive * (shift_time(alive, offset) if offset else alive)
    returns[...] = gained
    code[...] = reached


def scan_body(received, after, carried):
    del after
    shards, depth = carried.shape[0], carried.shape[1]
    held = max(1, depth // LANES)
    part = min(depth, LANES)
    end = received.shape[1]
    for q in range(held):
        state = jnp.zeros((part, LANES), F32)
        for j in range(shards):
            carried[j, q * part : (q + 1) * part] = state.astype(BF16)
            both = received[j, depth:end].astype(F32)
            high = both[end - depth - 2 * held + q : end - depth - 2 * held + q + 1]
            low = both[end - depth - held + q : end - depth - held + q + 1]
            state = (high + low) * state + received[j, q * part : (q + 1) * part].astype(F32)


def shift_time(x, distance):
    lane = lax.broadcasted_iota(jnp.int32, x.shape, 1)
    row = lax.broadcasted_iota(jnp.int32, x.shape, 0)
    count = x.shape[0]
    below = jnp.where(row < count - 1, pltpu.roll(x, count - 1, 0), 0.0)
    moved = jnp.where(lane < distance, below, x)
    return pltpu.roll(moved, LANES - distance, 1)


def inside_body(
    skip, inner, state, rows, cols, local, scores
):
    length = inner.shape[0]
    heads = rows.shape[0] // 3
    block = LANES
    readout = state[:, LANES:]
    writes = state[:, :LANES]
    scores[...] = dot(readout, writes, ((1,), (1,)))
    below = lax.broadcasted_iota(jnp.int32, (block, block), 0) >= lax.broadcasted_iota(
        jnp.int32, (block, block), 1
    )
    for h in range(heads):
        at = slice(h * LANES, (h + 1) * LANES)
        for r in range(0, length, block):
            here = jnp.broadcast_to(cols[r : r + block, heads + h : heads + h + 1], (block, LANES))
            pieces = []
            for s in range(0, r + block, block):
                gap = here - rows[h : h + 1, s : s + block]
                if s == r:
                    gap = jnp.where(below, gap, -jnp.inf)
                weight = scores[r : r + block, s : s + block] * rows[heads + h : heads + h + 1, s : s + block]
                pieces.append((jnp.exp(gap) * weight).astype(BF16))
            weights = jnp.concatenate(pieces, axis=1)
            out = dot(weights, inner[0 : r + block, at])
            out = out + skip[h] * inner[r : r + block, at].astype(F32)
            local[r : r + block, at] = out.astype(local.dtype)


def finish_body(state, carried, local, gate, cols, norm_gain, value_weight, message):
    length = state.shape[0]
    heads = carried.shape[0] // LANES
    block = LANES
    weight = norm_gain[...] * value_weight[...]
    squares, sums = [], []
    for r in range(0, length, block):
        readout = state[r : r + block, LANES:]
        square = jnp.zeros((block, LANES), F32)
        total = jnp.zeros((block, LANES), F32)
        for c in range(0, heads, 2):
            both = jnp.concatenate(
                [carried[(c + i) * LANES : (c + i + 1) * LANES] for i in range(2)], axis=1
            )
            fix = dot(readout, both)
            for i in range(2):
                h = c + i
                at = slice(h * LANES, (h + 1) * LANES)
                reach = cols[r : r + block, 2 * heads + h : 2 * heads + h + 1]
                mixed = local[r : r + block, at].astype(F32) + reach * fix[:, i * LANES : (i + 1) * LANES]
                gated = mixed * gate[r : r + block, at].astype(F32)
                square = square + gated * gated
                total = total + gated * weight[:, at]
        squares.append(jnp.sum(square.T, axis=0, keepdims=True))
        sums.append(jnp.sum(total.T, axis=0, keepdims=True))
    tile = jnp.concatenate(squares + sums, axis=0)
    for dest in range(message.shape[0]):
        message[dest] = tile


def loss_body(rank, received, returns, code, values, targets, loss, values_s, targets_s):
    devices, double, _ = received.shape
    per = double // 2
    total_rows = returns.shape[0]
    shards = total_rows // per
    group = devices // shards
    for j in range(shards):
        tile = received[group * j]
        for g in range(1, group):
            tile = tile + received[group * j + g]
        values_s[per * j : per * (j + 1)] = tile[per:] * lax.rsqrt(tile[:per] / D_INNER + EPSILON)
    value = values_s[...]
    reached = code[...]
    target = returns[...]
    for offset in range(1, NSTEP + 1):
        ahead = shift_time(value, offset)
        target = target + jnp.where(reached == offset, DISCOUNT**offset * ahead, 0.0)
    targets_s[...] = target
    residual = target - value
    terms = jnp.where(residual < 0, 1.0 - EXPECTILE, EXPECTILE) * residual * residual
    loss[...] = jnp.sum(jnp.sum(terms, axis=0, keepdims=True), axis=1, keepdims=True) / (
        total_rows * LANES
    )
    own = pl.ds(rank[0] * per, per)
    values[...] = values_s[own]
    targets[...] = targets_s[own]


def per_device(
    states,
    inner_weight,
    gate_weight,
    state_weight,
    step_weight,
    step_bias,
    decay_rate,
    skip_gain,
    conv_inner,
    conv_state,
    norm_gain,
    value_weight,
    rewards,
    done_flags,
    horizon,
):
    length = states.shape[0]
    heads = step_bias.shape[0]
    inner_width = inner_weight.shape[1]
    state_width = state_weight.shape[1]
    shards = lax.axis_size("seq")
    devices = shards * lax.axis_size("head")
    depth = heads * LANES // shards
    per = length // LANES
    packed = -(-(5 * per + 2 * max(1, depth // LANES)) // 8) * 8
    rank = lax.axis_index("seq").astype(jnp.int32).reshape(1)
    shape = jax.ShapeDtypeStruct
    done_row = done_flags.reshape(1, length)

    edge = call(
        edge_body,
        shape((HALO, states.shape[1]), BF16),
        [HBM],
        [pltpu.SemaphoreType.DMA(())],
        flops=2 * length * states.shape[1] * inner_width,
        moved=4 * states.size,
        name="edge",
    )(in_hbm(states))
    halo = lax.ppermute(edge, "seq", [(i, i + 1) for i in range(shards - 1)])
    inner_pre, state_pre, rows, cols = call(
        project_body,
        [
            shape((length, inner_width), BF16),
            shape((length, state_width), BF16),
            shape((3 * heads, length), F32),
            shape((length, LANES), F32),
        ],
        [SMEM, SMEM] + [VMEM] * 5,
        flops=2 * length * states.shape[1] * (inner_width + state_width),
        name="project",
    )(step_bias, decay_rate, done_row, states, step_weight.T, state_weight, inner_weight)
    inner, state, message = call(
        conv_body,
        [
            shape((length, inner_width), BF16),
            shape((length, state_width), BF16),
            shape((shards, depth + packed, LANES), BF16),
        ],
        [VMEM] * 12,
        [pltpu.VMEM((2, length + HALO, LANES), F32), pltpu.VMEM((length, inner_width), BF16)],
        flops=length * inner_width * 600,
        name="conv",
    )(
        halo,
        inner_weight,
        state_weight,
        inner_pre,
        state_pre,
        conv_inner,
        conv_state,
        rows,
        cols,
        rewards.reshape(1, length),
        done_row,
        horizon.reshape(1, length),
    )
    received = lax.all_to_all(message, "seq", 0, 0, tiled=True)
    local = call(
        inside_body,
        shape((length, inner_width), BF16),
        [SMEM] + [VMEM] * 4,
        [pltpu.VMEM((length, length), F32)],
        flops=length * length * inner_width * 4,
        name="inside",
    )(skip_gain, inner, state, rows, cols)
    carried = call(
        scan_body,
        shape((shards, depth, LANES), BF16),
        [VMEM, ANY],
        name="scan",
    )(received, local)
    entered = lax.all_to_all(carried, "seq", 0, 0, tiled=True).reshape(heads * LANES, LANES)
    trajectory = shape((shards * per, LANES), F32)
    gate, returns, code = call(
        gate_body,
        [shape((length, inner_width), BF16), trajectory, trajectory],
        [SMEM, HBM, HBM, VMEM, ANY],
        [pltpu.VMEM(states.shape, BF16), pltpu.VMEM(gate_weight.shape, BF16)]
        + [pltpu.VMEM((shards * per, LANES), F32)] * 3
        + [pltpu.SemaphoreType.DMA((2,))],
        flops=2 * length * states.shape[1] * inner_width,
        name="gate",
    )(rank, in_hbm(states), in_hbm(gate_weight), received, carried)
    parts = call(
        finish_body,
        shape((devices, 2 * per, LANES), F32),
        [VMEM] * 7,
        flops=length * inner_width * 300,
        name="finish",
    )(
        state,
        entered,
        local,
        gate,
        cols,
        norm_gain.reshape(1, inner_width),
        value_weight.reshape(1, inner_width),
    )
    everything = lax.all_to_all(parts, ("seq", "head"), 0, 0, tiled=True)
    own = shape((per, LANES), F32)
    values, targets, value_loss = call(
        loss_body,
        [own, own, shape((1, 1), F32)],
        [SMEM] + [VMEM] * 3,
        [pltpu.VMEM((shards * per, LANES), F32)] * 2,
        name="loss",
    )(rank, everything, returns, code)
    return values.reshape(length), targets.reshape(length), value_loss.reshape(())


def solution(mesh):
    placed = (
        P("seq", None),
        P(None, "head"),
        P(None, "head"),
        P(),
        P(None, "head"),
        P("head"),
        P("head"),
        P("head"),
        P(None, "head"),
        P(),
        P("head"),
        P("head"),
        P("seq"),
        P("seq"),
        P("seq"),
    )
    return jax.shard_map(
        per_device, mesh=mesh, in_specs=placed, out_specs=(P("seq"), P("seq"), P()), check_vma=False
    )
```

```python
import functools

import jax
import jax.numpy as jnp
from jax import lax
from jax.experimental import pallas as pl
from jax.experimental.pallas import tpu as pltpu
from jax.sharding import PartitionSpec as P

D_INNER = 4096
NSTEP = 8
DISCOUNT = 0.99
EXPECTILE = 0.7
EPSILON = 1e-05
LANES = 128
HALO = 8
CONV_ROWS = 32
RESET = 300.0
VMEM = pl.BlockSpec(memory_space=pltpu.VMEM)
SMEM = pl.BlockSpec(memory_space=pltpu.SMEM)
ANY = pl.BlockSpec(memory_space=pl.ANY)
HBM = pl.BlockSpec(memory_space=pltpu.HBM)
F32 = jnp.float32
BF16 = jnp.bfloat16


def call(body, outs, ins, scratch=(), flops=0, moved=0, name=None, limit=10, alias=None):
    return pl.pallas_call(
        body,
        out_shape=outs,
        in_specs=ins,
        out_specs=jax.tree.map(lambda _: VMEM, outs),
        scratch_shapes=list(scratch),
        input_output_aliases=alias or {},
        cost_estimate=pl.CostEstimate(flops=flops, transcendentals=0, bytes_accessed=moved),
        compiler_params=pltpu.CompilerParams(vmem_limit_bytes=limit * 2**20),
        name=name,
    )


def in_hbm(x):
    return pltpu.with_memory_space_constraint(x, pltpu.HBM)


def dot(a, b, dims=((1,), (0,))):
    return lax.dot_general(a, b, (dims, ((), ())), preferred_element_type=F32)


def silu(x):
    return x * jax.nn.sigmoid(x)


def column(scalars, count, shape):
    row = lax.broadcasted_iota(jnp.int32, shape, 0)
    out = jnp.zeros(shape, F32)
    for h in range(count):
        out = jnp.where(row == h, scalars[h], out)
    return out


def edge_body(states_hbm, edge, arrived):
    rows = pl.ds(states_hbm.shape[0] - HALO, HALO)
    copy = pltpu.make_async_copy(states_hbm.at[rows], edge, arrived)
    copy.start()
    copy.wait()


def project_body(
    bias, decay, done, states, step_w, state_w, inner_w, inner_pre, state_pre, rows, cols
):
    length = states.shape[0]
    heads = bias.shape[0]
    width = 2 * LANES
    for c in range(0, state_w.shape[1], width):
        state_pre[:, c : c + width] = dot(states[...], state_w[:, c : c + width]).astype(BF16)
    for c in range(0, inner_w.shape[1], width):
        if c == width:
            step_rows(bias, decay, done, states, step_w, rows, cols, heads, length)
        inner_pre[:, c : c + width] = dot(states[...], inner_w[:, c : c + width]).astype(BF16)


def step_rows(bias, decay, done, states, step_w, rows, cols, heads, length):
    shape = (heads, length)
    step = dot(step_w[...], states[...], ((1,), (1,))) + column(bias, heads, shape)
    step = jnp.maximum(step, 0.0) + jnp.log1p(jnp.exp(-jnp.abs(step)))
    ended = jnp.broadcast_to(done[...].astype(F32) * RESET, shape)
    total = -column(decay, heads, shape) * step - ended
    lane = lax.broadcasted_iota(jnp.int32, shape, 1)
    stride = 1
    while stride < length:
        total = total + jnp.where(lane >= stride, pltpu.roll(total, stride, 1), 0.0)
        stride *= 2
    reach = total + ended
    last = total[:, length - 1 :]
    rows[0:heads] = reach
    rows[heads : 2 * heads] = step
    rows[2 * heads :] = jnp.broadcast_to(jnp.exp(last), shape)
    tail = jnp.exp(last - reach) * step
    fill = jnp.zeros((LANES - 3 * heads, length), F32)
    cols[...] = jnp.concatenate([tail, reach, jnp.exp(reach), fill], axis=0).T


def conv_body(
    halo,
    inner_w,
    state_w,
    inner_pre,
    state_pre,
    taps_inner,
    taps_state,
    rows,
    cols,
    rewards,
    done,
    horizon,
    inner,
    state,
    message,
    pad,
    weighted,
):
    length = inner_pre.shape[0]
    heads = rows.shape[0] // 3
    shards = message.shape[0]
    depth = heads * LANES // shards
    block = CONV_ROWS

    def convolve(rim, source, taps, target, c, scaled):
        slot = pad.at[c % 2]
        at = slice(c * LANES, (c + 1) * LANES)
        slot[0:HALO] = rim
        for r in range(0, length, block):
            here = source[r : r + block, at].astype(F32)
            slot[r + HALO : r + HALO + block] = here
            out = taps[3:4, at] * here
            for k in range(3):
                out = out + taps[k : k + 1, at] * slot[r + HALO - 3 + k : r + HALO - 3 + k + block]
            out = silu(out).astype(BF16)
            target[r : r + block, at] = out
            if scaled:
                scale = cols[r : r + block, c : c + 1]
                weighted[r : r + block, at] = (out.astype(F32) * scale).astype(BF16)

    rim = dot(halo[...], state_w[...]).astype(BF16).astype(F32)
    for c in range(state_pre.shape[1] // LANES):
        convolve(rim[:, c * LANES : (c + 1) * LANES], state_pre, taps_state, state, c, False)
    writes = state[:, :LANES].astype(F32).T.astype(BF16)
    pair = 2 * LANES
    for c in range(0, heads, 2):
        at = slice(c * LANES, c * LANES + pair)
        rim = dot(halo[...], inner_w[:, at]).astype(BF16).astype(F32)
        convolve(rim[:, :LANES], inner_pre, taps_inner, inner, c, True)
        convolve(rim[:, LANES:], inner_pre, taps_inner, inner, c + 1, True)
        summary = dot(writes, weighted[:, at]).astype(BF16)
        for half in range(2):
            own = summary[:, half * LANES : (half + 1) * LANES]
            first = (c + half) * LANES
            step = min(depth, LANES)
            for q in range(0, LANES, step):
                dest, at_row = divmod(first + q, depth)
                message[dest, at_row : at_row + step] = own[q : q + step]
    total = rows[2 * heads :, 0:LANES]
    high = total.astype(BF16).astype(F32)
    low = total - high
    per = length // LANES
    reward = lane_rows(rewards, per)
    first = reward.astype(BF16).astype(F32)
    second = (reward - first).astype(BF16).astype(F32)
    series = [first, second, reward - first - second, lane_rows(done, per), lane_rows(horizon, per)]
    held = max(1, depth // LANES)
    spare = message.shape[1] - depth - 5 * per - 2 * held
    if spare:
        series.append(jnp.zeros((spare, LANES), F32))
    for dest in range(shards):
        head = dest * depth // LANES
        decays = [high[head : head + held], low[head : head + held]]
        message[dest, depth:] = jnp.concatenate(series + decays, axis=0).astype(BF16)


def lane_rows(ref, count):
    pieces = [ref[:, q * LANES : (q + 1) * LANES].astype(F32) for q in range(count)]
    return jnp.concatenate(pieces, axis=0)


def gate_body(
    rank,
    states_hbm,
    gate_hbm,
    received,
    after,
    local,
    cols,
    near,
    far,
    returns,
    code,
    states,
    gate_w,
    reward_s,
    alive_s,
    steps_s,
    arrived,
):
    del rank
    pairs = [(gate_hbm, gate_w), (states_hbm, states)]
    copies = [pltpu.make_async_copy(*pair, arrived.at[i]) for i, pair in enumerate(pairs)]
    for copy in copies:
        copy.start()
    depth = after.shape[1]
    series(received, depth, states.shape[0] // LANES, returns, code, reward_s, alive_s, steps_s)
    for copy in copies:
        copy.wait()
    width = 2 * LANES
    heads = gate_w.shape[1] // LANES
    for c in range(0, gate_w.shape[1], width):
        pre = dot(states[...], gate_w[:, c : c + width]).astype(BF16).astype(F32)
        gate = silu(pre)
        near[:, c : c + width] = (local[:, c : c + width].astype(F32) * gate).astype(BF16)
        for half in range(0, width, LANES):
            lane = 2 * heads + (c + half) // LANES
            scaled = gate[:, half : half + LANES] * cols[:, lane : lane + 1]
            far[:, c + half : c + half + LANES] = scaled.astype(BF16)


def series(received, depth, per, returns, code, reward_s, alive_s, steps_s):
    shards = received.shape[0]
    for j in range(shards):
        extra = received[j, depth:].astype(F32)
        to = slice(j * per, (j + 1) * per)
        reward_s[to] = extra[0:per] + extra[per : 2 * per] + extra[2 * per : 3 * per]
        alive_s[to] = 1.0 - extra[3 * per : 4 * per]
        steps_s[to] = extra[4 * per : 5 * per]
    reward, alive, steps = reward_s[...], alive_s[...], steps_s[...]
    gained = jnp.zeros(reward.shape, F32)
    survive = jnp.ones(reward.shape, F32)
    reached = jnp.zeros(reward.shape, F32)
    for offset in range(NSTEP + 1):
        ahead = shift_time(reward, offset) if offset else reward
        gained = gained + jnp.where(offset < steps, DISCOUNT**offset * survive * ahead, 0.0)
        reached = jnp.where(offset == steps, survive * offset, reached)
        if offset < NSTEP:
            survive = survive * (shift_time(alive, offset) if offset else alive)
    returns[...] = gained
    code[...] = reached


def scan_body(received, after, carried):
    del after
    shards, depth = carried.shape[0], carried.shape[1]
    held = max(1, depth // LANES)
    part = min(depth, LANES)
    end = received.shape[1]
    for q in range(held):
        state = jnp.zeros((part, LANES), F32)
        for j in range(shards):
            carried[j, q * part : (q + 1) * part] = state.astype(BF16)
            both = received[j, depth:end].astype(F32)
            high = both[end - depth - 2 * held + q : end - depth - 2 * held + q + 1]
            low = both[end - depth - held + q : end - depth - held + q + 1]
            state = (high + low) * state + received[j, q * part : (q + 1) * part].astype(F32)


def shift_time(x, distance):
    lane = lax.broadcasted_iota(jnp.int32, x.shape, 1)
    row = lax.broadcasted_iota(jnp.int32, x.shape, 0)
    count = x.shape[0]
    below = jnp.where(row < count - 1, pltpu.roll(x, count - 1, 0), 0.0)
    moved = jnp.where(lane < distance, below, x)
    return pltpu.roll(moved, LANES - distance, 1)


def inside_body(
    skip, inner, state, rows, cols, local, scores
):
    length = inner.shape[0]
    heads = rows.shape[0] // 3
    block = LANES
    readout = state[:, LANES:]
    writes = state[:, :LANES]
    scores[...] = dot(readout, writes, ((1,), (1,)))
    below = lax.broadcasted_iota(jnp.int32, (block, block), 0) >= lax.broadcasted_iota(
        jnp.int32, (block, block), 1
    )
    for h in range(heads):
        at = slice(h * LANES, (h + 1) * LANES)
        for r in range(0, length, block):
            here = jnp.broadcast_to(cols[r : r + block, heads + h : heads + h + 1], (block, LANES))
            pieces = []
            for s in range(0, r + block, block):
                gap = here - rows[h : h + 1, s : s + block]
                if s == r:
                    gap = jnp.where(below, gap, -jnp.inf)
                weight = scores[r : r + block, s : s + block] * rows[heads + h : heads + h + 1, s : s + block]
                pieces.append((jnp.exp(gap) * weight).astype(BF16))
            weights = jnp.concatenate(pieces, axis=1)
            out = dot(weights, inner[0 : r + block, at])
            out = out + skip[h] * inner[r : r + block, at].astype(F32)
            local[r : r + block, at] = out.astype(local.dtype)


def finish_body(state, carried, near, far, norm_gain, value_weight, message):
    length = state.shape[0]
    heads = carried.shape[0] // LANES
    block = LANES
    weight = norm_gain[...] * value_weight[...]
    squares, sums = [], []
    for r in range(0, length, block):
        readout = state[r : r + block, LANES:]
        square = jnp.zeros((block, LANES), F32)
        total = jnp.zeros((block, LANES), F32)
        for c in range(0, heads, 2):
            both = jnp.concatenate(
                [carried[(c + i) * LANES : (c + i + 1) * LANES] for i in range(2)], axis=1
            )
            fix = dot(readout, both)
            for i in range(2):
                h = c + i
                at = slice(h * LANES, (h + 1) * LANES)
                fixed = far[r : r + block, at].astype(F32) * fix[:, i * LANES : (i + 1) * LANES]
                gated = near[r : r + block, at].astype(F32) + fixed
                square = square + gated * gated
                total = total + gated * weight[:, at]
        squares.append(jnp.sum(square.T, axis=0, keepdims=True))
        sums.append(jnp.sum(total.T, axis=0, keepdims=True))
    tile = jnp.concatenate(squares + sums, axis=0)
    for dest in range(message.shape[0]):
        message[dest] = tile


def loss_body(rank, received, returns, code, values, targets, loss, values_s, targets_s):
    devices, double, _ = received.shape
    per = double // 2
    total_rows = returns.shape[0]
    shards = total_rows // per
    group = devices // shards
    for j in range(shards):
        tile = received[group * j]
        for g in range(1, group):
            tile = tile + received[group * j + g]
        values_s[per * j : per * (j + 1)] = tile[per:] * lax.rsqrt(tile[:per] / D_INNER + EPSILON)
    value = values_s[...]
    reached = code[...]
    target = returns[...]
    for offset in range(1, NSTEP + 1):
        ahead = shift_time(value, offset)
        target = target + jnp.where(reached == offset, DISCOUNT**offset * ahead, 0.0)
    targets_s[...] = target
    residual = target - value
    terms = jnp.where(residual < 0, 1.0 - EXPECTILE, EXPECTILE) * residual * residual
    loss[...] = jnp.sum(jnp.sum(terms, axis=0, keepdims=True), axis=1, keepdims=True) / (
        total_rows * LANES
    )
    own = pl.ds(rank[0] * per, per)
    values[...] = values_s[own]
    targets[...] = targets_s[own]


def per_device(
    states,
    inner_weight,
    gate_weight,
    state_weight,
    step_weight,
    step_bias,
    decay_rate,
    skip_gain,
    conv_inner,
    conv_state,
    norm_gain,
    value_weight,
    rewards,
    done_flags,
    horizon,
):
    length = states.shape[0]
    heads = step_bias.shape[0]
    inner_width = inner_weight.shape[1]
    state_width = state_weight.shape[1]
    shards = lax.axis_size("seq")
    devices = shards * lax.axis_size("head")
    depth = heads * LANES // shards
    per = length // LANES
    packed = -(-(5 * per + 2 * max(1, depth // LANES)) // 8) * 8
    rank = lax.axis_index("seq").astype(jnp.int32).reshape(1)
    shape = jax.ShapeDtypeStruct
    done_row = done_flags.reshape(1, length)

    edge = call(
        edge_body,
        shape((HALO, states.shape[1]), BF16),
        [HBM],
        [pltpu.SemaphoreType.DMA(())],
        flops=2 * length * states.shape[1] * inner_width,
        moved=4 * states.size,
        name="edge",
    )(in_hbm(states))
    halo = lax.ppermute(edge, "seq", [(i, i + 1) for i in range(shards - 1)])
    inner_pre, state_pre, rows, cols = call(
        project_body,
        [
            shape((length, inner_width), BF16),
            shape((length, state_width), BF16),
            shape((3 * heads, length), F32),
            shape((length, LANES), F32),
        ],
        [SMEM, SMEM] + [VMEM] * 5,
        flops=2 * length * states.shape[1] * (inner_width + state_width),
        name="project",
    )(step_bias, decay_rate, done_row, states, step_weight.T, state_weight, inner_weight)
    inner, state, message = call(
        conv_body,
        [
            shape((length, inner_width), BF16),
            shape((length, state_width), BF16),
            shape((shards, depth + packed, LANES), BF16),
        ],
        [VMEM] * 12,
        [pltpu.VMEM((2, length + HALO, LANES), F32), pltpu.VMEM((length, inner_width), BF16)],
        flops=length * inner_width * 600,
        name="conv",
    )(
        halo,
        inner_weight,
        state_weight,
        inner_pre,
        state_pre,
        conv_inner,
        conv_state,
        rows,
        cols,
        rewards.reshape(1, length),
        done_row,
        horizon.reshape(1, length),
    )
    received = lax.all_to_all(message, "seq", 0, 0, tiled=True)
    local = call(
        inside_body,
        shape((length, inner_width), BF16),
        [SMEM] + [VMEM] * 4,
        [pltpu.VMEM((length, length), F32)],
        flops=length * length * inner_width * 4,
        name="inside",
    )(skip_gain, inner, state, rows, cols)
    carried = call(
        scan_body,
        shape((shards, depth, LANES), BF16),
        [VMEM, ANY],
        name="scan",
    )(received, local)
    entered = lax.all_to_all(carried, "seq", 0, 0, tiled=True).reshape(heads * LANES, LANES)
    trajectory = shape((shards * per, LANES), F32)
    wide = shape((length, inner_width), BF16)
    near, far, returns, code = call(
        gate_body,
        [wide, wide, trajectory, trajectory],
        [SMEM, HBM, HBM, VMEM, ANY, VMEM, VMEM],
        [pltpu.VMEM(states.shape, BF16), pltpu.VMEM(gate_weight.shape, BF16)]
        + [pltpu.VMEM((shards * per, LANES), F32)] * 3
        + [pltpu.SemaphoreType.DMA((2,))],
        flops=2 * length * states.shape[1] * inner_width,
        name="gate",
        alias={5: 0},
    )(rank, in_hbm(states), in_hbm(gate_weight), received, carried, local, cols)
    parts = call(
        finish_body,
        shape((devices, 2 * per, LANES), F32),
        [VMEM] * 6,
        flops=length * inner_width * 300,
        name="finish",
    )(
        state,
        entered,
        near,
        far,
        norm_gain.reshape(1, inner_width),
        value_weight.reshape(1, inner_width),
    )
    everything = lax.all_to_all(parts, ("seq", "head"), 0, 0, tiled=True)
    own = shape((per, LANES), F32)
    values, targets, value_loss = call(
        loss_body,
        [own, own, shape((1, 1), F32)],
        [SMEM] + [VMEM] * 3,
        [pltpu.VMEM((shards * per, LANES), F32)] * 2,
        name="loss",
    )(rank, everything, returns, code)
    return values.reshape(length), targets.reshape(length), value_loss.reshape(())


def solution(mesh):
    placed = (
        P("seq", None),
        P(None, "head"),
        P(None, "head"),
        P(),
        P(None, "head"),
        P("head"),
        P("head"),
        P("head"),
        P(None, "head"),
        P(),
        P("head"),
        P("head"),
        P("seq"),
        P("seq"),
        P("seq"),
    )
    return jax.shard_map(
        per_device, mesh=mesh, in_specs=placed, out_specs=(P("seq"), P("seq"), P()), check_vma=False
    )
```
